32 devices in a mesh: dp: 8 (over y, x, core), seq: 4 (over z).
Axes of the slice: x: 2, y: 2, z: 4, core: 2. Of those that a mesh axis runs over, the one named last changes fastest.
Arguments:
- grad_rows: bfloat16 [8, 320, 4, 1280], P('dp', 'seq'), may hold values from -6 to 6
- row_owner: int32 [8, 320, 1], P('dp', 'seq'), may hold values from 0 to 3; in each aligned block of 80 rows (0 to 79, 80 to 159, ..., all dimensions but the last counted through in order) at most 25 rows name the same one
- acts: bfloat16 [8, 4, 100, 4, 1280], P('dp', 'seq'), may hold values from -6 to 6
- xact: bfloat16 [8, 4, 100, 4, 1280], P('dp', 'seq'), may hold values from -72 to 72
- gamma: float32 [1280], replicated, may hold values from 0.25 to 1.75
- w_out: bfloat16 [1280, 1280], replicated, may hold values from -0.15625 to 0.15625
Outputs:
- attn_grad: bfloat16 [8, 4, 100, 4, 1280], P('dp', 'seq')
- weight_grad: float32 [1280, 1280], P('dp')
- gain_grad: float32 [1280], replicated
The draws below stay inside these ranges and needn't reach their ends.
Inputs may be any that keep to these rules, and one draw needn't show every extreme that they name: `row_owner`: within the rows of one device (each aligned block of 80 rows) no owner is named more than 25 times, a bound that some block reaches.
All inputs are finite; a program needn't handle non-finite values.
Results may differ from the reference program's by a relative error of at most 0.0049.
Values may be sent and summed in bfloat16 or wider, within the bound.
A program may use at most 64 MiB of HBM per device.

```python
import math
import jax
import jax.numpy as jnp
import numpy as np
from jax import lax

DV = 1280
PM = 4
TOK_DEV = 80
CAP = 25
SLOTS = 100
SEQ = 320
N_DP = 8
N_SEQ = 4


def draw_xact(key, part):
    full_shape = (N_DP, N_SEQ, SLOTS, PM, DV)
    key_base, key_rows, key_cols = jax.random.split(jax.random.fold_in(key, 17), 3)
    row_scale = jnp.exp(jax.random.uniform(key_rows, (N_DP, N_SEQ, SLOTS, PM, 1), jnp.float32, jnp.log(0.5), jnp.log(6.0)))
    col_scale = jnp.exp(jax.random.uniform(key_cols, (DV,), jnp.float32, jnp.log(0.3), jnp.log(3.0)))
    values = jnp.clip(jax.random.normal(key_base, full_shape, jnp.float32), -4.0, 4.0)
    return (values * row_scale * col_scale).astype(jnp.bfloat16)


def spiked(values, rng, source, target, parts, factor):
    def block_of(axis_at):
        return (jnp.arange(values.shape[axis_at]) // (values.shape[axis_at] // parts)).reshape((-1,) + (1,) * (values.ndim - 1 - axis_at))

    first = jax.random.permutation(rng, parts)[block_of(target)]
    far = (block_of(target) + parts // 2) % parts
    return jnp.where((block_of(source) == first) | (block_of(source) == far), factor * values, values)


def block_levels(stream_key, shape, cuts, smallest, high):
    def one(dim, shards_of):
        draws = jax.random.uniform(jax.random.fold_in(jax.random.fold_in(stream_key, 6), dim), (shards_of,), jnp.float32, smallest / len(cuts), high / len(cuts))
        return jnp.repeat(jnp.exp(draws), shape[dim] // shards_of).reshape((-1,) + (1,) * (len(shape) - dim - 1))

    level = one(*cuts[0])
    for cut in cuts[1:]:
        level = level * one(*cut)
    return level


def deal_out(own_key, own, number, rows, amount, top, reach, slope):
    sequence = jax.random.permutation(own_key, amount)
    crowded, ordinary = shares(amount, rows * top, reach, slope, True), shares(amount, rows * top, reach, slope, False)
    places = jnp.arange(amount)

    def named(sizes, turn):
        used = int((sizes > 0).sum())
        fixed = max(1, used // 4)
        moved = fixed + (places - fixed + turn * (used - fixed)) % max(1, amount - fixed)
        return jnp.zeros((amount,), jnp.int32).at[sequence[jnp.where(places < fixed, places, moved)]].set(jnp.asarray(sizes, jnp.int32))

    sizes = jnp.where(number % 4 == 0, named(crowded, number // 4), named(ordinary, number - number // 4 - 1))
    mixed = jax.random.permutation(jax.random.fold_in(own, 3), amount)
    giver, taker = mixed[0:amount // 2 * 2:2], mixed[1:amount // 2 * 2:2]
    margin = jnp.minimum(sizes[giver] - 1, reach - sizes[taker]) // 2
    margin = jnp.where((giver == sequence[0]) | (taker == sequence[0]) | (sizes[taker] == 0), 0, jnp.maximum(margin, 0))
    moved = jax.random.randint(jax.random.fold_in(own, 4), (amount // 2,), 0, 1 << 20) % (margin + 1)
    sizes = sizes.at[giver].add(-moved).at[taker].add(moved)
    labels = jnp.searchsorted(jnp.cumsum(sizes), jnp.arange(rows * top), side="right").astype(jnp.int32)
    listing = labels.reshape(top, rows).T
    listing = listing[jax.random.permutation(jax.random.fold_in(own, 1), rows)]
    turn = jax.random.randint(jax.random.fold_in(own, 2), (rows, 1), 0, top)
    return jnp.take_along_axis(listing, (jnp.arange(top)[None, :] + turn) % top, axis=1)


def shares(amount, total, most, slope, full):
    portions = [(1 << 20) // math.isqrt(grade ** slope) + 1 for grade in range(1, amount + 1)]
    largest = most if full else min(most, max(-(-total // amount), total * portions[0] // sum(portions)))
    least = 1 if total - largest >= amount - 1 else 0
    counts, spare = [largest] + [least] * (amount - 1), total - largest - least * (amount - 1)
    while spare > 0:
        free = [i for i in range(1, amount) if counts[i] < largest] or [i for i in range(1, amount) if counts[i] < most]
        whole, left = sum([portions[i] for i in free]), spare
        for i in free:
            addition = min(most - counts[i], max(1, left * portions[i] // whole), spare)
            counts[i] = counts[i] + addition
            spare = spare - addition
    return np.array(counts)


def scatter_about(key, shape, width, reach, cuts=(), kind=jnp.bfloat16):
    values = jax.random.normal(key, shape, jnp.float32) * width
    if len(cuts) > 0:
        values = block_levels(key, shape, cuts, -0.22, 0.18) * values
    return jnp.clip(values, min=-reach, max=reach).astype(kind)


def gaussian_with(key, dims, width, bound, shards, heavy, held_as=jnp.bfloat16):
    entries = width * jax.random.normal(key, dims, jnp.float32)
    if shards:
        entries = entries * block_levels(key, dims, shards, -0.22, 0.18)
    return jnp.clip(spiked(entries, jax.random.fold_in(key, 3), *heavy), -bound, bound).astype(held_as)


def setup_inputs(seed: int = 0) -> dict:
    splits = jax.random.split(jax.random.key(seed), 7)
    grad_rows = scatter_about(splits[0], (N_DP, SEQ, PM, DV), 1.0, 6.0, ((0, 8), (1, 4)))
    row_owner_keys = jax.random.split(jax.random.fold_in(splits[1], 1), N_DP * SEQ // TOK_DEV)
    row_owner_turns = jax.random.permutation(jax.random.fold_in(splits[1], 3), N_DP * SEQ // TOK_DEV)
    row_owner = jax.vmap(lambda own, number: deal_out(jax.random.fold_in(splits[1], 2), own, number, TOK_DEV, N_SEQ, 1, CAP, 2))(row_owner_keys, row_owner_turns).reshape((N_DP, SEQ, 1))
    acts = gaussian_with(splits[2], (N_DP, N_SEQ, SLOTS, PM, DV), 1.0, 6.0, ((0, 8), (1, 4)), (0, 4, 8, 2.0))
    xact = draw_xact(jax.random.fold_in(splits[6], 71), 0)
    gamma = jnp.clip(1.0 + 0.15 * jax.random.normal(splits[4], (DV,), jnp.float32), 0.25, 1.75)
    w_out = scatter_about(splits[5], (DV, DV), DV ** -0.5, 0.15625)
    return dict(grad_rows=grad_rows, row_owner=row_owner, acts=acts, xact=xact, gamma=gamma, w_out=w_out)


epsilon = 1e-06

def slot_table(owners, buckets, capacity):
    picked = (owners[:, None] == jnp.arange(buckets, dtype=jnp.int32)[None, :]).astype(jnp.int32)
    before = jnp.cumsum(picked, axis=0) - picked
    ranking = lax.optimization_barrier(jnp.sum(before * picked, axis=1)).astype(jnp.int32)
    target = owners.astype(jnp.int32) * capacity + ranking
    places = jnp.arange(buckets * capacity, dtype=jnp.int32)
    return (places[:, None] == target[None, :]).astype(jnp.bfloat16)

def norm_backward(upstream, inputs, gamma):
    values = inputs.astype(jnp.float32)
    inverse = lax.rsqrt(lax.optimization_barrier(jnp.mean(values * values, axis=1, keepdims=True)) + epsilon)
    normed = values * inverse
    gradient = upstream.astype(jnp.float32)
    gain_part = lax.optimization_barrier(jnp.sum(gradient * normed, axis=0))
    scaled = gamma.astype(jnp.float32) * gradient
    centre = lax.optimization_barrier(jnp.mean(scaled * normed, axis=1, keepdims=True))
    patch_grad = (inverse * (scaled - normed * centre)).astype(jnp.bfloat16)
    return (patch_grad, gain_part)

def reference(grad_rows, row_owner, acts, xact, gamma, w_out):

    def place(owner_block, row_block):
        placing = slot_table(owner_block, N_SEQ, CAP)
        return jnp.dot(placing, row_block, preferred_element_type=jnp.float32).astype(jnp.bfloat16)

    def group_terms(carry, group):
        grad_group, owner_group, acts_group, xact_group = group
        owners = owner_group[:, 0].reshape(N_SEQ, TOK_DEV)
        row_blocks = grad_group.reshape(N_SEQ, TOK_DEV, PM * DV)
        outgoing = jax.vmap(place)(owners, row_blocks).reshape(N_SEQ, N_SEQ, CAP, PM * DV)
        received = jnp.swapaxes(outgoing, 0, 1).reshape(N_SEQ * SLOTS * PM, DV)
        act_rows = acts_group.reshape(N_SEQ * SLOTS * PM, DV)
        patch_grad, gain_part = norm_backward(received, xact_group.reshape(N_SEQ * SLOTS * PM, DV), gamma)
        attn = lax.dot_general(patch_grad, w_out, (((1,), (1,)), ((), ())), preferred_element_type=jnp.float32).astype(jnp.bfloat16)
        weight_part = lax.dot_general(act_rows, patch_grad, (((0,), (0,)), ((), ())), preferred_element_type=jnp.float32)
        return ((carry[0] + weight_part, carry[1] + gain_part), attn.reshape(N_SEQ, SLOTS, PM, DV))
    initial = (jnp.zeros((DV, DV), jnp.float32), jnp.zeros((DV,), jnp.float32))
    totals, attn_grad = lax.scan(group_terms, initial, (grad_rows, row_owner, acts, xact))
    weight_raw, gain_raw = totals
    norm_total = jnp.sqrt(jnp.sum(weight_raw * weight_raw) + jnp.sum(gain_raw * gain_raw) + epsilon)
    factor = jnp.float32(DV) / norm_total
    return (attn_grad, weight_raw * factor, gain_raw * factor)
```

```python
import functools

import jax
import jax.numpy as jnp
from jax import lax
from jax.experimental import pallas as pl
from jax.experimental.pallas import tpu as pltpu
from jax.sharding import PartitionSpec as P

epsilon = 1e-06
MESH = pl.DeviceIdType.MESH


def round_up(value, unit):
    return -(-value // unit) * unit


def exchange(axis, count, me, source, landing, send_sems, recv_sems):
    def copy(k, place):
        return pltpu.make_async_remote_copy(
            src_ref=source,
            dst_ref=landing.at[place],
            send_sem=send_sems.at[k],
            recv_sem=recv_sems.at[k],
            device_id={axis: lax.rem(me + k, count)},
            device_id_type=MESH,
        )

    def start():
        for k in range(1, count):
            copy(k, me).start()

    def wait():
        for k in range(1, count):
            copy(k, lax.rem(me - k + count, count)).wait()

    return start, wait


def scatter(axis, count, me, source, landing, send_sems, recv_sems):
    def copy(k, place):
        peer = lax.rem(me + k, count)
        return pltpu.make_async_remote_copy(
            src_ref=source.at[peer],
            dst_ref=landing.at[place],
            send_sem=send_sems.at[k],
            recv_sem=recv_sems.at[k],
            device_id={axis: peer},
            device_id_type=MESH,
        )

    def start():
        for k in range(1, count):
            copy(k, me).start()

    return start, lambda k: copy(k, lax.rem(me - k + count, count)).wait()


def kernel(
    dims, owner_row, owner_col, grad, acts, xact, gamma, w_out, attn, weight, gain, scratch
):
    n_dp, n_seq, bits, splits, patches, chunk, used, orders = dims
    dp = lax.axis_index("dp")
    seq = lax.axis_index("seq")
    block = acts.shape[1]
    features = acts.shape[2]
    rows = features // n_dp
    part = rows // splits

    barrier = pltpu.get_barrier_semaphore()
    for k in range(1, n_dp):
        pl.semaphore_signal(
            barrier, inc=1, device_id={"dp": lax.rem(dp + k, n_dp)}, device_id_type=MESH
        )
    for k in range(1, n_seq):
        pl.semaphore_signal(
            barrier, inc=1, device_id={"seq": lax.rem(seq + k, n_seq)}, device_id_type=MESH
        )

    tokens = grad.shape[0]
    earlier = lax.broadcasted_iota(jnp.int32, (tokens, tokens), 0)
    later = lax.broadcasted_iota(jnp.int32, (tokens, tokens), 1)
    same = (
        (owner_col[...] == owner_row[...])
        & (earlier < later)
        & (lax.rem(later - earlier + tokens * patches, patches) == 0)
    )
    rank = jnp.sum(jnp.where(same, 1.0, 0.0), axis=0, keepdims=True)
    patch = lax.rem(lax.broadcasted_iota(jnp.int32, (1, tokens), 1), patches)
    target = rank * patches + patch.astype(jnp.float32)
    place = lax.broadcasted_iota(jnp.int32, (block, tokens), 0).astype(jnp.float32)

    def fill(dest, carry):
        here = jnp.where(owner_row[...] == dest, target, -1.0)
        placing = jnp.where(place == here, 1.0, 0.0).astype(jnp.bfloat16)
        scratch["outgoing"][dest] = jnp.dot(
            placing, grad[...], preferred_element_type=jnp.float32
        ).astype(jnp.bfloat16)
        return carry

    lax.fori_loop(0, n_seq, fill, 0)
    pl.semaphore_wait(barrier, n_dp - 1 + n_seq - 1)
    start_rows, wait_rows = scatter(
        "seq", n_seq, seq, scratch["outgoing"], scratch["received"], *scratch["row_sems"]
    )
    start_rows()
    scratch["received"][seq] = scratch["outgoing"][seq]

    gain_part = jnp.zeros((1, features), jnp.float32)
    for k in range(n_seq):
        if k > 0:
            wait_rows(k)
        origin = lax.rem(seq - k + n_seq, n_seq)
        values = xact[origin].astype(jnp.float32)
        inverse = lax.rsqrt(jnp.mean(values * values, axis=1, keepdims=True) + epsilon)
        normed = values * inverse
        gradient = scratch["received"][origin].astype(jnp.float32)
        gain_part += jnp.sum(gradient * normed, axis=0, keepdims=True)
        scaled = gamma[...] * gradient
        centre = jnp.mean(scaled * normed, axis=1, keepdims=True)
        scratch["patch"][origin] = (inverse * (scaled - normed * centre)).astype(jnp.bfloat16)

    gain_own, gain_dp, gain_mid, gain_seq = scratch["gain"]
    gain_own[...] = gain_part
    gain_dp[dp] = gain_part
    start_gain, wait_gain = exchange("dp", n_dp, dp, gain_own, gain_dp, *scratch["gain_sems"][0])
    start_gain()

    width = 256 if features % 256 == 0 else 128
    depth = n_seq * block

    @pl.loop(0, features // width)
    def _(step):
        columns = pl.ds(pl.multiple_of(step * width, width), width)
        product = lax.dot_general(
            acts[...].reshape(depth, features),
            scratch["patch"][:, :, columns].reshape(depth, width),
            (((0,), (0,)), ((), ())),
            preferred_element_type=jnp.float32,
        )
        for device in range(n_dp):
            for h in range(splits):
                place = 0
                for b in orders[h]:
                    place = place * 2 + (device >> b) % 2
                half = n_dp // 2
                first = device * rows + h * part
                scratch["sums"][h][0][place // half, place % half, :, columns] = product[
                    first : first + part
                ]

    def attn_rows():
        @pl.loop(0, features // width)
        def _(step):
            columns = pl.ds(pl.multiple_of(step * width, width), width)
            product = lax.dot_general(
                scratch["patch"][...].reshape(depth, features),
                w_out[columns, :],
                (((1,), (1,)), ((), ())),
                preferred_element_type=jnp.float32,
            )
            attn[:, :, columns] = product.astype(jnp.bfloat16).reshape(n_seq, block, width)

    for i in range(bits):
        copies = []
        for h in range(splits):
            b = orders[h][i]
            mine = lax.rem(dp // (1 << b), 2)
            sent, landed, sems = scratch["halves"][h][i]
            sums = scratch["sums"][h][i]
            sent[...] = sums[1 - mine].astype(jnp.bfloat16)
            copy = pltpu.make_async_remote_copy(
                src_ref=sent,
                dst_ref=landed,
                send_sem=sems.at[0],
                recv_sem=sems.at[1],
                device_id={"dp": dp + (1 - 2 * mine) * (1 << b)},
                device_id_type=MESH,
            )
            copy.start()
            copies.append((copy, sums, mine, landed))
        if i == min(1, bits - 1):
            attn_rows()
            wait_gain()
            gain_mid[...] = jnp.sum(gain_dp[...], axis=0)
            gain_seq[seq] = gain_mid[...]
            start_gain, wait_gain = exchange(
                "seq", n_seq, seq, gain_mid, gain_seq, *scratch["gain_sems"][1]
            )
            start_gain()
        for h in range(splits):
            copy, sums, mine, landed = copies[h]
            copy.wait()
            total = sums[mine] + landed[...].astype(jnp.float32)
            if i + 1 < bits:
                half = total.shape[0] // 2
                following = scratch["sums"][h][i + 1]
                following[0] = total[:half]
                following[1] = total[half:]
            else:
                scratch["reduced"][h * part : (h + 1) * part] = total[0]

    chunk_own, chunk_sent, chunk_landed, chunk_all, chunk_mine = scratch["chunks"]
    for s in range(n_seq):
        if s < used:
            piece = scratch["reduced"][s * chunk : (s + 1) * chunk]
            chunk_own[s] = piece
            chunk_sent[s] = piece.astype(jnp.bfloat16)
        else:
            chunk_own[s] = jnp.zeros((chunk, features), jnp.float32)
            chunk_sent[s] = jnp.zeros((chunk, features), jnp.bfloat16)
    start_chunks, wait_chunks = scatter(
        "seq", n_seq, seq, chunk_sent, chunk_landed, *scratch["chunk_sems"][0]
    )
    start_chunks()
    wait_gain()
    gain_total = jnp.sum(gain_seq[...], axis=0)
    total = chunk_own[seq]
    for k in range(1, n_seq):
        wait_chunks(k)
        total += chunk_landed[lax.rem(seq - k + n_seq, n_seq)].astype(jnp.float32)
    rounded = total.astype(jnp.bfloat16)
    chunk_mine[...] = rounded
    chunk_all[seq] = rounded
    start_all, wait_all = exchange(
        "seq", n_seq, seq, chunk_mine, chunk_all, *scratch["chunk_sems"][1]
    )
    start_all()
    square_own, square_dp, square_mid, square_seq = scratch["square"]
    squares = jnp.sum(total * total, axis=0, keepdims=True)
    square_own[...] = squares
    square_dp[dp] = squares
    start_square, wait_square = exchange(
        "dp", n_dp, dp, square_own, square_dp, *scratch["square_sems"][0]
    )
    start_square()
    wait_square()
    squares = jnp.sum(square_dp[...], axis=0)
    square_mid[...] = squares
    square_seq[seq] = squares
    start_square, wait_square = exchange(
        "seq", n_seq, seq, square_mid, square_seq, *scratch["square_sems"][1]
    )
    start_square()
    wait_square()
    squares = jnp.sum(square_seq[...], axis=0) + gain_total * gain_total
    norm = jnp.sqrt(jnp.sum(squares, axis=1, keepdims=True) + epsilon)
    factor = jnp.float32(features) / norm
    gain[...] = gain_total * factor
    wait_all()
    for s in range(used):
        weight[s * chunk : (s + 1) * chunk] = chunk_all[s].astype(jnp.float32) * factor


def on_device(grad_rows, row_owner, acts, xact, gamma, w_out):
    n_dp = lax.axis_size("dp")
    n_seq = lax.axis_size("seq")
    slot_count, patches, features = acts.shape[2:]
    tokens = grad_rows.shape[1]
    capacity = slot_count // n_seq
    taken = capacity * patches
    block = round_up(taken, 16 if taken % 16 == 0 else 8)
    rows = features // n_dp
    bits = n_dp.bit_length() - 1
    assert 1 << bits == n_dp
    splits = 2 if rows % 32 == 0 and bits > 2 else 1
    part = rows // splits
    chunk = round_up(-(-rows // n_seq), 8)
    used = rows // chunk
    orders = [list(range(bits)), [0] + list(range(bits - 1, 0, -1))][:splits]
    dims = (n_dp, n_seq, bits, splits, patches, chunk, used, orders)

    def padded(slots):
        flat = slots.reshape(n_seq, taken, features)
        return jnp.pad(flat, ((0, 0), (0, block - taken), (0, 0)))

    owners = jnp.repeat(row_owner.reshape(tokens), patches)
    dma = pltpu.SemaphoreType.DMA

    def sem_pair(count):
        return [dma((count,)), dma((count,))]

    bf16, f32 = jnp.bfloat16, jnp.float32

    def vector_set():
        line = (1, features)
        return [
            pltpu.VMEM(line, f32),
            pltpu.VMEM((n_dp,) + line, f32),
            pltpu.VMEM(line, f32),
            pltpu.VMEM((n_seq,) + line, f32),
        ]

    halves, sums = [], []
    for h in range(splits):
        halves.append([])
        sums.append([])
        for i in range(bits):
            size = n_dp >> (i + 1)
            sums[h].append(pltpu.VMEM((2, size, part, features), f32))
            halves[h].append(
                [
                    pltpu.VMEM((size, part, features), bf16),
                    pltpu.VMEM((size, part, features), bf16),
                    dma((2,)),
                ]
            )
    scratch = dict(
        outgoing=pltpu.VMEM((n_seq, block, features), bf16),
        received=pltpu.VMEM((n_seq, block, features), bf16),
        row_sems=sem_pair(n_seq),
        patch=pltpu.VMEM((n_seq, block, features), bf16),
        gain=vector_set(),
        gain_sems=[sem_pair(n_dp), sem_pair(n_seq)],
        square=vector_set(),
        square_sems=[sem_pair(n_dp), sem_pair(n_seq)],
        sums=sums,
        halves=halves,
        reduced=pltpu.VMEM((rows, features), f32),
        chunks=[
            pltpu.VMEM((n_seq, chunk, features), f32),
            pltpu.VMEM((n_seq, chunk, features), bf16),
            pltpu.VMEM((n_seq, chunk, features), bf16),
            pltpu.VMEM((n_seq, chunk, features), bf16),
            pltpu.VMEM((chunk, features), bf16),
        ],
        chunk_sems=[sem_pair(n_seq), sem_pair(n_seq)],
    )
    flat_scratch, tree = jax.tree.flatten(scratch)
    n_in, n_out = 7, 3

    def body(*refs):
        kernel(dims, *refs[: n_in + n_out], jax.tree.unflatten(tree, refs[n_in + n_out :]))

    vmem = pl.BlockSpec(memory_space=pltpu.VMEM)
    attn, weight, gain = pl.pallas_call(
        body,
        out_shape=(
            jax.ShapeDtypeStruct((n_seq, block, features), bf16),
            jax.ShapeDtypeStruct((rows, features), f32),
            jax.ShapeDtypeStruct((1, features), f32),
        ),
        in_specs=[vmem] * n_in,
        out_specs=(vmem,) * n_out,
        scratch_shapes=flat_scratch,
        compiler_params=pltpu.CompilerParams(
            collective_id=0, has_side_effects=True, vmem_limit_bytes=60 * 1024 * 1024
        ),
        name="backward",
    )(
        owners[None, :],
        owners[:, None],
        grad_rows.reshape(tokens * patches, features),
        padded(acts),
        padded(xact),
        gamma[None, :],
        w_out,
    )
    return (attn[:, :taken].reshape(acts.shape), weight, gain.reshape(features))


def solution(mesh):
    return jax.shard_map(
        on_device,
        mesh=mesh,
        in_specs=(
            P("dp", "seq", None, None),
            P("dp", "seq", None),
            P("dp", "seq", None, None, None),
            P("dp", "seq", None, None, None),
            P(),
            P(),
        ),
        out_specs=(P("dp", "seq", None, None, None), P("dp", None), P()),
        check_vma=False,
    )
```

```python
import functools

import jax
import jax.numpy as jnp
from jax import lax
from jax.experimental import pallas as pl
from jax.experimental.pallas import tpu as pltpu
from jax.sharding import PartitionSpec as P

epsilon = 1e-06
MESH = pl.DeviceIdType.MESH


def round_up(value, unit):
    return -(-value // unit) * unit


def exchange(axis, count, me, source, landing, send_sems, recv_sems):
    def copy(k, place):
        return pltpu.make_async_remote_copy(
            src_ref=source,
            dst_ref=landing.at[place],
            send_sem=send_sems.at[k],
            recv_sem=recv_sems.at[k],
            device_id={axis: lax.rem(me + k, count)},
            device_id_type=MESH,
        )

    def start():
        for k in range(1, count):
            copy(k, me).start()

    def wait():
        for k in range(1, count):
            copy(k, lax.rem(me - k + count, count)).wait()

    return start, wait


def scatter(axis, count, me, source, landing, send_sems, recv_sems):
    def copy(k, place):
        peer = lax.rem(me + k, count)
        return pltpu.make_async_remote_copy(
            src_ref=source.at[peer],
            dst_ref=landing.at[place],
            send_sem=send_sems.at[k],
            recv_sem=recv_sems.at[k],
            device_id={axis: peer},
            device_id_type=MESH,
        )

    def start():
        for k in range(1, count):
            copy(k, me).start()

    return start, lambda k: copy(k, lax.rem(me - k + count, count)).wait()


def kernel(
    dims, owner, grad, acts_hbm, xact_hbm, gamma, w_hbm, attn_hbm, weight_hbm, gain, scratch
):
    n_dp, n_seq, bits, splits, chunk, used, orders, width = dims
    dp = lax.axis_index("dp")
    seq = lax.axis_index("seq")
    capacity, patches, features = scratch["outgoing"].shape[1:]
    taken = capacity * patches
    depth = n_seq * taken
    rows = features // n_dp
    part = rows // splits
    columns = features // width
    direct = scratch["direct"]

    local_sems = scratch["local_sems"]
    acts, xact, w_out, attn, weight = scratch["local"]
    loads = [
        pltpu.make_async_copy(source, target, local_sems.at[i])
        for i, (source, target) in enumerate(
            ((xact_hbm, xact), (acts_hbm, acts), (w_hbm, w_out))
        )
    ]
    for load in loads:
        load.start()

    barrier = pltpu.get_barrier_semaphore()

    def greet(device):
        pl.semaphore_signal(barrier, inc=1, device_id=device, device_id_type=MESH)

    if direct:
        me = dp * n_seq + seq
        peers = n_dp * n_seq - 1
        for k in range(1, n_dp * n_seq):
            peer = lax.rem(me + k, n_dp * n_seq)
            greet({"dp": peer // n_seq, "seq": lax.rem(peer, n_seq)})
    else:
        peers = n_dp - 1 + n_seq - 1
        for k in range(1, n_dp):
            greet({"dp": lax.rem(dp + k, n_dp)})
        for k in range(1, n_seq):
            greet({"seq": lax.rem(seq + k, n_seq)})

    f32 = jnp.float32
    tokens = grad.shape[0]
    flat = tokens * patches
    spread = (
        lax.broadcasted_iota(jnp.int32, (tokens, flat), 0)
        == lax.broadcasted_iota(jnp.int32, (tokens, flat), 1) // patches
    )
    spread = jnp.where(spread, 1.0, 0.0)
    owners = jnp.broadcast_to(owner[...].astype(f32), (8, tokens))
    owner_row = jnp.dot(owners, spread, preferred_element_type=f32)[0:1]
    owner_col = lax.dot_general(
        spread, owners, (((0,), (1,)), ((), ())), preferred_element_type=f32
    )[:, 0:1]
    earlier = lax.broadcasted_iota(jnp.int32, (flat, flat), 0)
    later = lax.broadcasted_iota(jnp.int32, (flat, flat), 1)
    same = (
        (owner_col == owner_row)
        & (earlier < later)
        & (lax.rem(later - earlier + flat, patches) == 0)
    )
    rank = jnp.sum(jnp.where(same, 1.0, 0.0), axis=0, keepdims=True)
    patch = lax.rem(lax.broadcasted_iota(jnp.int32, (1, flat), 1), patches)
    target = owner_row * taken + rank * patches + patch.astype(f32)
    place = lax.broadcasted_iota(jnp.int32, (depth, flat), 0).astype(f32)
    placing = jnp.where(place == target, 1.0, 0.0).astype(jnp.bfloat16)
    scratch["outgoing"][...] = (
        jnp.dot(placing, grad[...].reshape(flat, features), preferred_element_type=f32)
        .astype(jnp.bfloat16)
        .reshape(n_seq, capacity, patches, features)
    )
    pl.semaphore_wait(barrier, peers)
    start_rows, wait_rows = scatter(
        "seq", n_seq, seq, scratch["outgoing"], scratch["received"], *scratch["row_sems"]
    )
    start_rows()
    scratch["received"][seq] = scratch["outgoing"][seq]
    loads[1].wait()
    scratch["turned"][...] = acts[...].reshape(depth, features).T
    loads[0].wait()

    gain_part = jnp.zeros((1, features), f32)
    for k in sorted(range(n_seq), key=lambda k: min(k, n_seq - k)):
        if k > 0:
            wait_rows(k)
        origin = lax.rem(seq - k + n_seq, n_seq)
        values = xact[origin].astype(f32).reshape(taken, features)
        inverse = lax.rsqrt(jnp.mean(values * values, axis=1, keepdims=True) + epsilon)
        normed = values * inverse
        gradient = scratch["received"][origin].astype(f32).reshape(taken, features)
        gain_part += jnp.sum(gradient * normed, axis=0, keepdims=True)
        scaled = gamma[...].reshape(1, features) * gradient
        centre = jnp.mean(scaled * normed, axis=1, keepdims=True)
        patch_grad = inverse * (scaled - normed * centre)
        scratch["patch"][origin] = patch_grad.reshape(capacity, patches, features).astype(
            jnp.bfloat16
        )
    scratch["flat"][...] = scratch["patch"][...].reshape(depth, features)

    def over_both(value, buffers, sems):
        own, all_dp, middle, all_seq = buffers
        own[...] = value
        all_dp[dp] = value
        start_dp, wait_dp = exchange("dp", n_dp, dp, own, all_dp, *sems[0])
        start_seq, wait_seq = exchange("seq", n_seq, seq, middle, all_seq, *sems[1])
        start_dp()

        def turn():
            wait_dp()
            middle[...] = jnp.sum(all_dp[...], axis=0)
            all_seq[seq] = middle[...]
            start_seq()

        def finish():
            wait_seq()
            return jnp.sum(all_seq[...], axis=0)

        return turn, finish

    def over_all(value, own, landing, sems):
        total = n_dp * n_seq
        own[...] = value
        landing[me] = value

        def copy(k, place):
            peer = lax.rem(me + k, total)
            return pltpu.make_async_remote_copy(
                src_ref=own,
                dst_ref=landing.at[place],
                send_sem=sems[0].at[k],
                recv_sem=sems[1].at[k],
                device_id={"dp": peer // n_seq, "seq": lax.rem(peer, n_seq)},
                device_id_type=MESH,
            )

        for k in range(1, total):
            copy(k, me).start()
        for k in range(1, total):
            copy(k, lax.rem(me - k + total, total)).wait()
        return jnp.sum(landing[...], axis=0)

    turn_gain, finish_gain = over_both(gain_part, scratch["gain"], scratch["gain_sems"])

    chunk_own, chunk_sent, chunk_landed, chunk_all, chunk_mine = scratch["chunks"]
    squares = [jnp.zeros((1, width), f32)]

    def halve(c, h, i):
        b = orders[h][i]
        mine = lax.rem(dp // (1 << b), 2)
        sent, landed, send_sems, recv_sems = scratch["halves"][h][i]
        copy = pltpu.make_async_remote_copy(
            src_ref=sent.at[c],
            dst_ref=landed.at[c],
            send_sem=send_sems.at[c],
            recv_sem=recv_sems.at[c],
            device_id={"dp": dp + (1 - 2 * mine) * (1 << b)},
            device_id_type=MESH,
        )
        return copy, scratch["sums"][h][i], mine, sent, landed

    def send_half(c, h, i):
        copy, sums, mine, sent, landed = halve(c, h, i)
        sent[c] = sums[c, 1 - mine].astype(jnp.bfloat16)
        copy.start()

    def received_half(c, h, i):
        copy, sums, mine, sent, landed = halve(c, h, i)
        copy.wait()
        return sums[c, mine] + landed[c].astype(f32)

    def rows_out(c):
        return scatter(
            "seq", n_seq, seq, chunk_sent.at[c], chunk_landed.at[c],
            *[sems.at[c] for sems in scratch["chunk_sems"][0]]
        )

    def rows_back(c):
        return exchange(
            "seq", n_seq, seq, chunk_mine.at[c], chunk_all.at[c],
            *[sems.at[c] for sems in scratch["chunk_sems"][1]]
        )

    def stage(c, i):
        span = slice(c * width, (c + 1) * width)
        if i == 0:
            product = jnp.dot(
                scratch["turned"][...], scratch["flat"][:, span], preferred_element_type=f32
            )
            half = n_dp // 2
            for device in range(n_dp):
                for h in range(splits):
                    place = 0
                    for b in orders[h]:
                        place = place * 2 + (device >> b) % 2
                    first = device * rows + h * part
                    scratch["sums"][h][0][c, place // half, place % half] = product[
                        first : first + part
                    ]
            for h in range(splits):
                send_half(c, h, 0)
        elif i < bits:
            for h in range(splits):
                total = received_half(c, h, i - 1)
                half = total.shape[0] // 2
                scratch["sums"][h][i][c, 0] = total[:half]
                scratch["sums"][h][i][c, 1] = total[half:]
                send_half(c, h, i)
        elif i == bits:
            for h in range(splits):
                scratch["reduced"][c, h * part : (h + 1) * part] = received_half(c, h, i - 1)[0]
            for s in range(n_seq):
                if s < used:
                    piece = scratch["reduced"][c, s * chunk : (s + 1) * chunk]
                else:
                    piece = jnp.zeros((chunk, width), f32)
                chunk_own[c, s] = piece
                chunk_sent[c, s] = piece.astype(jnp.bfloat16)
            rows_out(c)[0]()
        elif i == bits + 1:
            total = chunk_own[c, seq]
            for k in range(1, n_seq):
                rows_out(c)[1](k)
                total += chunk_landed[c, lax.rem(seq - k + n_seq, n_seq)].astype(f32)
            rounded = total.astype(jnp.bfloat16)
            chunk_mine[c] = rounded
            chunk_all[c, seq] = rounded
            rows_back(c)[0]()
            squares[0] = squares[0] + jnp.sum(total * total, axis=0, keepdims=True)

    def attn_columns(c):
        span = slice(c * width, (c + 1) * width)
        product = lax.dot_general(
            scratch["flat"][...], w_out[span, :], (((1,), (1,)), ((), ())),
            preferred_element_type=f32,
        )
        attn[:, :, :, span] = product.astype(jnp.bfloat16).reshape(
            n_seq, capacity, patches, width
        )

    stages = bits + 2
    attn_copy = pltpu.make_async_copy(attn, attn_hbm, local_sems.at[3])
    for t in range(columns + stages - 1):
        for i in range(stages):
            if 0 <= t - i < columns:
                stage(t - i, i)
        if t == 1:
            turn_gain()
            loads[2].wait()
        if 0 <= t - 2 < columns:
            attn_columns(t - 2)
            if t - 2 == columns - 1:
                attn_copy.start()
    gain_total = finish_gain()

    line = squares[0][:, 0:128]
    for lane in range(128, width, 128):
        line = line + squares[0][:, lane : lane + 128]
    if direct:
        line = over_all(line, *scratch["square"], scratch["square_sems"])
    else:
        turn_square, finish_square = over_both(line, scratch["square"], scratch["square_sems"])
        turn_square()
        line = finish_square()
    norm = jnp.sqrt(
        jnp.sum(line, axis=1, keepdims=True)
        + jnp.sum(gain_total * gain_total, axis=1, keepdims=True)
        + epsilon
    )
    factor = jnp.float32(features) / norm
    gain[...] = (gain_total * factor).reshape(features)
    for c in range(columns):
        rows_back(c)[1]()
        for s in range(used):
            weight[s * chunk : (s + 1) * chunk, c * width : (c + 1) * width] = (
                chunk_all[c, s].astype(f32) * factor
            )
    weight_copy = pltpu.make_async_copy(weight, weight_hbm, local_sems.at[4])
    weight_copy.start()
    attn_copy.wait()
    weight_copy.wait()


def on_device(grad_rows, row_owner, acts, xact, gamma, w_out):
    n_dp = lax.axis_size("dp")
    n_seq = lax.axis_size("seq")
    slot_count, patches, features = acts.shape[2:]
    tokens = grad_rows.shape[1]
    capacity = slot_count // n_seq
    depth = slot_count * patches
    rows = features // n_dp
    bits = n_dp.bit_length() - 1
    assert 1 << bits == n_dp
    splits = 2 if rows % 32 == 0 and bits > 2 else 1
    part = rows // splits
    chunk = round_up(-(-rows // n_seq), 8)
    used = rows // chunk
    width = 256 if features % 256 == 0 else 128
    columns = features // width
    orders = [list(range(bits)), [0] + list(range(bits - 1, 0, -1))][:splits]
    dims = (n_dp, n_seq, bits, splits, chunk, used, orders, width)
    direct = n_dp * n_seq <= 64

    dma = pltpu.SemaphoreType.DMA
    bf16, f32 = jnp.bfloat16, jnp.float32

    def sem_pair(*counts):
        return [dma(counts), dma(counts)]

    def vector_set(size):
        line = (1, size)
        return [
            pltpu.VMEM(line, f32),
            pltpu.VMEM((n_dp,) + line, f32),
            pltpu.VMEM(line, f32),
            pltpu.VMEM((n_seq,) + line, f32),
        ]

    halves, sums = [], []
    for h in range(splits):
        halves.append([])
        sums.append([])
        for i in range(bits):
            size = n_dp >> (i + 1)
            sums[h].append(pltpu.VMEM((columns, 2, size, part, width), f32))
            moved = pltpu.VMEM((columns, size, part, width), bf16)
            halves[h].append([moved, moved] + sem_pair(columns))
    slots = (n_seq, capacity, patches, features)
    scratch = dict(
        local_sems=dma((5,)),
        local=[
            pltpu.VMEM(slots, bf16),
            pltpu.VMEM(slots, bf16),
            pltpu.VMEM((features, features), bf16),
            pltpu.VMEM(slots, bf16),
            pltpu.VMEM((rows, features), f32),
        ],
        outgoing=pltpu.VMEM(slots, bf16),
        received=pltpu.VMEM(slots, bf16),
        row_sems=sem_pair(n_seq),
        patch=pltpu.VMEM(slots, bf16),
        flat=pltpu.VMEM((depth, features), bf16),
        turned=pltpu.VMEM((features, depth), bf16),
        gain=vector_set(features),
        gain_sems=[sem_pair(n_dp), sem_pair(n_seq)],
        sums=sums,
        halves=halves,
        reduced=pltpu.VMEM((columns, rows, width), f32),
        chunks=[
            pltpu.VMEM((columns, n_seq, chunk, width), f32),
            pltpu.VMEM((columns, n_seq, chunk, width), bf16),
            pltpu.VMEM((columns, n_seq, chunk, width), bf16),
            pltpu.VMEM((columns, n_seq, chunk, width), bf16),
            pltpu.VMEM((columns, chunk, width), bf16),
        ],
        chunk_sems=[sem_pair(columns, n_seq), sem_pair(columns, n_seq)],
    )
    if direct:
        scratch["square"] = [
            pltpu.VMEM((1, 128), f32), pltpu.VMEM((n_dp * n_seq, 1, 128), f32)
        ]
        scratch["square_sems"] = sem_pair(n_dp * n_seq)
    else:
        scratch["square"] = vector_set(128)
        scratch["square_sems"] = [sem_pair(n_dp), sem_pair(n_seq)]
    flat_scratch, tree = jax.tree.flatten(scratch)
    n_in, n_out = 6, 3

    def body(*refs):
        held = jax.tree.unflatten(tree, refs[n_in + n_out :])
        kernel(dims, *refs[: n_in + n_out], dict(held, direct=direct))

    vmem = pl.BlockSpec(memory_space=pltpu.VMEM)
    anywhere = pl.BlockSpec(memory_space=pl.ANY)
    attn, weight, gain = pl.pallas_call(
        body,
        out_shape=(
            jax.ShapeDtypeStruct(slots, bf16),
            jax.ShapeDtypeStruct((rows, features), f32),
            jax.ShapeDtypeStruct((features,), f32),
        ),
        in_specs=[vmem, vmem, anywhere, anywhere, vmem, anywhere],
        out_specs=(anywhere, anywhere, vmem),
        scratch_shapes=flat_scratch,
        compiler_params=pltpu.CompilerParams(
            collective_id=0, has_side_effects=True, vmem_limit_bytes=60 * 1024 * 1024
        ),
        name="backward",
    )(
        row_owner.reshape(1, tokens),
        grad_rows.reshape(tokens, patches, features),
        acts.reshape(slots),
        xact.reshape(slots),
        gamma,
        w_out,
    )
    return (attn.reshape(acts.shape), weight, gain)


def solution(mesh):
    return jax.shard_map(
        on_device,
        mesh=mesh,
        in_specs=(
            P("dp", "seq", None, None),
            P("dp", "seq", None),
            P("dp", "seq", None, None, None),
            P("dp", "seq", None, None, None),
            P(),
            P(),
        ),
        out_specs=(P("dp", "seq", None, None, None), P("dp", None), P()),
        check_vma=False,
    )
```

```python
import functools

import jax
import jax.numpy as jnp
from jax import lax
from jax.experimental import pallas as pl
from jax.experimental.pallas import tpu as pltpu
from jax.sharding import PartitionSpec as P

epsilon = 1e-06
MESH = pl.DeviceIdType.MESH


def round_up(value, unit):
    return -(-value // unit) * unit


def exchange(axis, count, me, source, landing, send_sems, recv_sems):
    def copy(k, place):
        return pltpu.make_async_remote_copy(
            src_ref=source,
            dst_ref=landing.at[place],
            send_sem=send_sems.at[k],
            recv_sem=recv_sems.at[k],
            device_id={axis: lax.rem(me + k, count)},
            device_id_type=MESH,
        )

    def start():
        for k in range(1, count):
            copy(k, me).start()

    def wait():
        for k in range(1, count):
            copy(k, lax.rem(me - k + count, count)).wait()

    return start, wait


def scatter(axis, count, me, source, landing, send_sems, recv_sems):
    def copy(k, place):
        peer = lax.rem(me + k, count)
        return pltpu.make_async_remote_copy(
            src_ref=source.at[peer],
            dst_ref=landing.at[place],
            send_sem=send_sems.at[k],
            recv_sem=recv_sems.at[k],
            device_id={axis: peer},
            device_id_type=MESH,
        )

    def start():
        for k in range(1, count):
            copy(k, me).start()

    return start, lambda k: copy(k, lax.rem(me - k + count, count)).wait()


def kernel(
    dims, owner, grad, acts_hbm, xact_hbm, gamma, w_hbm, attn_hbm, weight_hbm, gain, scratch
):
    n_dp, n_seq, bits, splits, chunk, used, orders, width = dims
    dp = lax.axis_index("dp")
    seq = lax.axis_index("seq")
    capacity, patches, features = scratch["outgoing"].shape[1:]
    taken = capacity * patches
    depth = n_seq * taken
    rows = features // n_dp
    part = rows // splits
    columns = features // width
    direct = scratch["direct"]

    local_sems = scratch["local_sems"]
    acts, xact, w_out, attn, weight = scratch["local"]
    loads = [
        pltpu.make_async_copy(source, target, local_sems.at[i])
        for i, (source, target) in enumerate(
            ((xact_hbm, xact), (acts_hbm, acts), (w_hbm, w_out))
        )
    ]
    for load in loads:
        load.start()

    barrier = pltpu.get_barrier_semaphore()

    def greet(device):
        pl.semaphore_signal(barrier, inc=1, device_id=device, device_id_type=MESH)

    if direct:
        me = dp * n_seq + seq
        peers = n_dp * n_seq - 1
        for k in range(1, n_dp * n_seq):
            peer = lax.rem(me + k, n_dp * n_seq)
            greet({"dp": peer // n_seq, "seq": lax.rem(peer, n_seq)})
    else:
        peers = n_dp - 1 + n_seq - 1
        for k in range(1, n_dp):
            greet({"dp": lax.rem(dp + k, n_dp)})
        for k in range(1, n_seq):
            greet({"seq": lax.rem(seq + k, n_seq)})

    f32 = jnp.float32
    tokens = grad.shape[0]
    flat = tokens * patches
    spread = (
        lax.broadcasted_iota(jnp.int32, (tokens, flat), 0)
        == lax.broadcasted_iota(jnp.int32, (tokens, flat), 1) // patches
    )
    spread = jnp.where(spread, 1.0, 0.0)
    owners = jnp.broadcast_to(owner[...].astype(f32), (8, tokens))
    owner_row = jnp.dot(owners, spread, preferred_element_type=f32)[0:1]
    owner_col = lax.dot_general(
        spread, owners, (((0,), (1,)), ((), ())), preferred_element_type=f32
    )[:, 0:1]
    earlier = lax.broadcasted_iota(jnp.int32, (flat, flat), 0)
    later = lax.broadcasted_iota(jnp.int32, (flat, flat), 1)
    same = (
        (owner_col == owner_row)
        & (earlier < later)
        & (lax.rem(later - earlier + flat, patches) == 0)
    )
    rank = jnp.sum(jnp.where(same, 1.0, 0.0), axis=0, keepdims=True)
    patch = lax.rem(lax.broadcasted_iota(jnp.int32, (1, flat), 1), patches)
    target = owner_row * taken + rank * patches + patch.astype(f32)
    place = lax.broadcasted_iota(jnp.int32, (depth, flat), 0).astype(f32)
    placing = jnp.where(place == target, 1.0, 0.0).astype(jnp.bfloat16)
    scratch["outgoing"][...] = (
        jnp.dot(placing, grad[...].reshape(flat, features), preferred_element_type=f32)
        .astype(jnp.bfloat16)
        .reshape(n_seq, capacity, patches, features)
    )
    pl.semaphore_wait(barrier, peers)
    start_rows, wait_rows = scatter(
        "seq", n_seq, seq, scratch["outgoing"], scratch["received"], *scratch["row_sems"]
    )
    start_rows()
    scratch["received"][seq] = scratch["outgoing"][seq]
    loads[1].wait()
    scratch["turned"][...] = acts[...].reshape(depth, features).T
    loads[0].wait()

    gain_part = jnp.zeros((1, features), f32)
    for k in sorted(range(n_seq), key=lambda k: min(k, n_seq - k)):
        if k > 0:
            wait_rows(k)
        origin = lax.rem(seq - k + n_seq, n_seq)
        values = xact[origin].astype(f32).reshape(taken, features)
        inverse = lax.rsqrt(jnp.mean(values * values, axis=1, keepdims=True) + epsilon)
        normed = values * inverse
        gradient = scratch["received"][origin].astype(f32).reshape(taken, features)
        gain_part += jnp.sum(gradient * normed, axis=0, keepdims=True)
        scaled = gamma[...].reshape(1, features) * gradient
        centre = jnp.mean(scaled * normed, axis=1, keepdims=True)
        patch_grad = inverse * (scaled - normed * centre)
        scratch["patch"][origin] = patch_grad.reshape(capacity, patches, features).astype(
            jnp.bfloat16
        )
    scratch["flat"][...] = scratch["patch"][...].reshape(depth, features)

    def over_both(value, buffers, sems):
        own, all_dp, middle, all_seq = buffers
        own[...] = value
        all_dp[dp] = value
        start_dp, wait_dp = exchange("dp", n_dp, dp, own, all_dp, *sems[0])
        start_seq, wait_seq = exchange("seq", n_seq, seq, middle, all_seq, *sems[1])
        start_dp()

        def turn():
            wait_dp()
            middle[...] = jnp.sum(all_dp[...], axis=0)
            all_seq[seq] = middle[...]
            start_seq()

        def finish():
            wait_seq()
            return jnp.sum(all_seq[...], axis=0)

        return turn, finish

    def over_all(value, own, landing, sems):
        total = n_dp * n_seq
        own[...] = value
        landing[me] = value

        def copy(k, place):
            peer = lax.rem(me + k, total)
            return pltpu.make_async_remote_copy(
                src_ref=own,
                dst_ref=landing.at[place],
                send_sem=sems[0].at[k],
                recv_sem=sems[1].at[k],
                device_id={"dp": peer // n_seq, "seq": lax.rem(peer, n_seq)},
                device_id_type=MESH,
            )

        for k in range(1, total):
            copy(k, me).start()
        for k in range(1, total):
            copy(k, lax.rem(me - k + total, total)).wait()
        return jnp.sum(landing[...], axis=0)

    turn_gain, finish_gain = over_both(gain_part, scratch["gain"], scratch["gain_sems"])

    chunk_own, chunk_sent, chunk_landed, chunk_all, chunk_mine = scratch["chunks"]
    squares = [jnp.zeros((1, width), f32)]

    def halve(c, h, i):
        b = orders[h][i]
        mine = lax.rem(dp // (1 << b), 2)
        sent, landed, send_sems, recv_sems = scratch["halves"][h][i]
        copy = pltpu.make_async_remote_copy(
            src_ref=sent.at[c],
            dst_ref=landed.at[c],
            send_sem=send_sems.at[c],
            recv_sem=recv_sems.at[c],
            device_id={"dp": dp + (1 - 2 * mine) * (1 << b)},
            device_id_type=MESH,
        )
        return copy, scratch["sums"][h][i], mine, sent, landed

    def send_half(c, h, i):
        copy, sums, mine, sent, landed = halve(c, h, i)
        sent[c] = sums[c, 1 - mine].astype(jnp.bfloat16)
        copy.start()

    def received_half(c, h, i):
        copy, sums, mine, sent, landed = halve(c, h, i)
        copy.wait()
        return sums[c, mine] + landed[c].astype(f32)

    def rows_out(c):
        return scatter(
            "seq", n_seq, seq, chunk_sent.at[c], chunk_landed.at[c],
            *[sems.at[c] for sems in scratch["chunk_sems"][0]]
        )

    def rows_back(c):
        return exchange(
            "seq", n_seq, seq, chunk_mine.at[c], chunk_all.at[c],
            *[sems.at[c] for sems in scratch["chunk_sems"][1]]
        )

    def stage(c, i):
        span = slice(c * width, (c + 1) * width)
        if i == 0:
            product = jnp.dot(
                scratch["turned"][...], scratch["flat"][:, span], preferred_element_type=f32
            )
            half = n_dp // 2
            for device in range(n_dp):
                for h in range(splits):
                    place = 0
                    for b in orders[h]:
                        place = place * 2 + (device >> b) % 2
                    first = device * rows + h * part
                    scratch["sums"][h][0][c, place // half, place % half] = product[
                        first : first + part
                    ]
            for h in range(splits):
                send_half(c, h, 0)
        elif i < bits:
            for h in range(splits):
                total = received_half(c, h, i - 1)
                half = total.shape[0] // 2
                scratch["sums"][h][i][c, 0] = total[:half]
                scratch["sums"][h][i][c, 1] = total[half:]
                send_half(c, h, i)
        elif i == bits:
            for h in range(splits):
                scratch["reduced"][c, h * part : (h + 1) * part] = received_half(c, h, i - 1)[0]
            for s in range(n_seq):
                if s < used:
                    piece = scratch["reduced"][c, s * chunk : (s + 1) * chunk]
                else:
                    piece = jnp.zeros((chunk, width), f32)
                chunk_own[c, s] = piece
                chunk_sent[c, s] = piece.astype(jnp.bfloat16)
            rows_out(c)[0]()
        elif i == bits + 1:
            total = chunk_own[c, seq]
            for k in range(1, n_seq):
                rows_out(c)[1](k)
                total += chunk_landed[c, lax.rem(seq - k + n_seq, n_seq)].astype(f32)
            rounded = total.astype(jnp.bfloat16)
            chunk_mine[c] = rounded
            chunk_all[c, seq] = rounded
            rows_back(c)[0]()
            squares[0] = squares[0] + jnp.sum(total * total, axis=0, keepdims=True)

    def attn_columns(c):
        span = slice(c * width, (c + 1) * width)
        product = lax.dot_general(
            scratch["flat"][...], w_out[span, :], (((1,), (1,)), ((), ())),
            preferred_element_type=f32,
        )
        attn[:, :, :, span] = product.astype(jnp.bfloat16).reshape(
            n_seq, capacity, patches, width
        )

    stages = bits + 2
    attn_copy = pltpu.make_async_copy(attn, attn_hbm, local_sems.at[3])
    lags = [i + max(0, i - bits) for i in range(stages)]
    for t in range(columns + max(lags[-1], 2)):
        for i in range(stages):
            if 0 <= t - lags[i] < columns:
                stage(t - lags[i], i)
        if t == 1:
            turn_gain()
            loads[2].wait()
        if 0 <= t - 2 < columns:
            attn_columns(t - 2)
            if t - 2 == columns - 1:
                attn_copy.start()
    gain_total = finish_gain()

    line = squares[0][:, 0:128]
    for lane in range(128, width, 128):
        line = line + squares[0][:, lane : lane + 128]
    if direct:
        line = over_all(line, *scratch["square"], scratch["square_sems"])
    else:
        turn_square, finish_square = over_both(line, scratch["square"], scratch["square_sems"])
        turn_square()
        line = finish_square()
    norm = jnp.sqrt(
        jnp.sum(line, axis=1, keepdims=True)
        + jnp.sum(gain_total * gain_total, axis=1, keepdims=True)
        + epsilon
    )
    factor = jnp.float32(features) / norm
    gain[...] = (gain_total * factor).reshape(features)
    for c in range(columns):
        rows_back(c)[1]()
        for s in range(used):
            weight[s * chunk : (s + 1) * chunk, c * width : (c + 1) * width] = (
                chunk_all[c, s].astype(f32) * factor
            )
    weight_copy = pltpu.make_async_copy(weight, weight_hbm, local_sems.at[4])
    weight_copy.start()
    attn_copy.wait()
    weight_copy.wait()


def on_device(grad_rows, row_owner, acts, xact, gamma, w_out):
    n_dp = lax.axis_size("dp")
    n_seq = lax.axis_size("seq")
    slot_count, patches, features = acts.shape[2:]
    tokens = grad_rows.shape[1]
    capacity = slot_count // n_seq
    depth = slot_count * patches
    rows = features // n_dp
    bits = n_dp.bit_length() - 1
    assert 1 << bits == n_dp
    splits = 2 if rows % 32 == 0 and bits > 2 else 1
    part = rows // splits
    chunk = round_up(-(-rows // n_seq), 8)
    used = rows // chunk
    width = 256 if features % 256 == 0 else 128
    columns = features // width
    orders = [list(range(bits)), [0] + list(range(bits - 1, 0, -1))][:splits]
    dims = (n_dp, n_seq, bits, splits, chunk, used, orders, width)
    direct = n_dp * n_seq <= 64

    dma = pltpu.SemaphoreType.DMA
    bf16, f32 = jnp.bfloat16, jnp.float32

    def sem_pair(*counts):
        return [dma(counts), dma(counts)]

    def vector_set(size):
        line = (1, size)
        return [
            pltpu.VMEM(line, f32),
            pltpu.VMEM((n_dp,) + line, f32),
            pltpu.VMEM(line, f32),
            pltpu.VMEM((n_seq,) + line, f32),
        ]

    halves, sums = [], []
    for h in range(splits):
        halves.append([])
        sums.append([])
        for i in range(bits):
            size = n_dp >> (i + 1)
            sums[h].append(pltpu.VMEM((columns, 2, size, part, width), f32))
            moved = pltpu.VMEM((columns, size, part, width), bf16)
            halves[h].append([moved, moved] + sem_pair(columns))
    slots = (n_seq, capacity, patches, features)
    scratch = dict(
        local_sems=dma((5,)),
        local=[
            pltpu.VMEM(slots, bf16),
            pltpu.VMEM(slots, bf16),
            pltpu.VMEM((features, features), bf16),
            pltpu.VMEM(slots, bf16),
            pltpu.VMEM((rows, features), f32),
        ],
        outgoing=pltpu.VMEM(slots, bf16),
        received=pltpu.VMEM(slots, bf16),
        row_sems=sem_pair(n_seq),
        patch=pltpu.VMEM(slots, bf16),
        flat=pltpu.VMEM((depth, features), bf16),
        turned=pltpu.VMEM((features, depth), bf16),
        gain=vector_set(features),
        gain_sems=[sem_pair(n_dp), sem_pair(n_seq)],
        sums=sums,
        halves=halves,
        reduced=pltpu.VMEM((columns, rows, width), f32),
        chunks=[
            pltpu.VMEM((columns, n_seq, chunk, width), f32),
            pltpu.VMEM((columns, n_seq, chunk, width), bf16),
            pltpu.VMEM((columns, n_seq, chunk, width), bf16),
            pltpu.VMEM((columns, n_seq, chunk, width), bf16),
            pltpu.VMEM((columns, chunk, width), bf16),
        ],
        chunk_sems=[sem_pair(columns, n_seq), sem_pair(columns, n_seq)],
    )
    if direct:
        scratch["square"] = [
            pltpu.VMEM((1, 128), f32), pltpu.VMEM((n_dp * n_seq, 1, 128), f32)
        ]
        scratch["square_sems"] = sem_pair(n_dp * n_seq)
    else:
        scratch["square"] = vector_set(128)
        scratch["square_sems"] = [sem_pair(n_dp), sem_pair(n_seq)]
    flat_scratch, tree = jax.tree.flatten(scratch)
    n_in, n_out = 6, 3

    def body(*refs):
        held = jax.tree.unflatten(tree, refs[n_in + n_out :])
        kernel(dims, *refs[: n_in + n_out], dict(held, direct=direct))

    vmem = pl.BlockSpec(memory_space=pltpu.VMEM)
    anywhere = pl.BlockSpec(memory_space=pl.ANY)
    attn, weight, gain = pl.pallas_call(
        body,
        out_shape=(
            jax.ShapeDtypeStruct(slots, bf16),
            jax.ShapeDtypeStruct((rows, features), f32),
            jax.ShapeDtypeStruct((features,), f32),
        ),
        in_specs=[vmem, vmem, anywhere, anywhere, vmem, anywhere],
        out_specs=(anywhere, anywhere, vmem),
        scratch_shapes=flat_scratch,
        compiler_params=pltpu.CompilerParams(
            collective_id=0, has_side_effects=True, vmem_limit_bytes=60 * 1024 * 1024
        ),
        name="backward",
    )(
        row_owner.reshape(1, tokens),
        grad_rows.reshape(tokens, patches, features),
        acts.reshape(slots),
        xact.reshape(slots),
        gamma,
        w_out,
    )
    return (attn.reshape(acts.shape), weight, gain)


def solution(mesh):
    return jax.shard_map(
        on_device,
        mesh=mesh,
        in_specs=(
            P("dp", "seq", None, None),
            P("dp", "seq", None),
            P("dp", "seq", None, None, None),
            P("dp", "seq", None, None, None),
            P(),
            P(),
        ),
        out_specs=(P("dp", "seq", None, None, None), P("dp", None), P()),
        check_vma=False,
    )
```
